256 devices in a mesh: pb: 8 (over x, core), pq: 32 (over z, y).
Axes of the slice: x: 4, y: 4, z: 8, core: 2. Of those that a mesh axis runs over, the one named last changes fastest.
Arguments:
- chol_vv: bfloat16 [352, 1792, 1792], P('pb', 'pq'), may hold values from -6 to 6
- chol_ov: bfloat16 [352, 256, 1792], P('pb', 'pq'), may hold values from -6 to 6
- chol_oo: bfloat16 [352, 256, 256], P('pb', 'pq'), may hold values from -6 to 6
- chol_vo: bfloat16 [352, 256, 1792], P('pb', None, 'pq'), may hold values from -6 to 6
- amplitudes: bfloat16 [256, 1792], P(None, 'pq'), may hold values from -0.125 to 0.125
Outputs:
- dressed: bfloat16 [352, 256, 1792], P('pb', 'pq')
- fock_ov: float32 [256, 1792], P('pq')
The draws below stay inside these ranges and needn't reach their ends.
All inputs are finite; a program needn't handle non-finite values.
Results may differ from the reference program's by a relative error of at most 0.0081.
Values may be sent and summed in bfloat16 or wider, within the bound.
A program may use at most 64 MiB of HBM per device.

```python
import jax
import jax.numpy as jnp
from jax import lax

NOCC = 256
NVIRT = 1792
QB = 44
NQ = 352
N_PB = 8


def levels(rng, dims, cuts, low, top_value):
    loudness, own = 1.0, jax.random.fold_in(rng, 6)
    for dim, shards_of in cuts:
        heights = jnp.exp(jax.random.uniform(jax.random.fold_in(own, dim), (shards_of,), jnp.float32, low / len(cuts), top_value / len(cuts)))
        loudness = loudness * jnp.repeat(heights, dims[dim] // shards_of).reshape([-1 if axis == dim else 1 for axis in range(len(dims))])
    return loudness


def noise(own_key, dims, spread, bound, split=(), dtype=jnp.bfloat16):
    drawn = jax.random.normal(own_key, dims, jnp.float32) * spread
    if len(split) > 0:
        drawn = levels(own_key, dims, split, -0.22, 0.18) * drawn
    return jnp.clip(drawn, min=-bound, max=bound).astype(dtype)


def setup_inputs(seed: int = 0) -> dict:
    splits = jax.random.split(jax.random.key(seed), 6)
    chol_vv = noise(splits[0], (NQ, NVIRT, NVIRT), 1.0, 6.0, ((0, 8), (1, 32)))
    chol_ov = noise(splits[1], (NQ, NOCC, NVIRT), 1.0, 6.0, ((0, 8), (1, 32)))
    chol_oo = noise(splits[2], (NQ, NOCC, NOCC), 1.0, 6.0, ((0, 8), (1, 32)))
    chol_vo = noise(splits[3], (NQ, NOCC, NVIRT), 1.0, 6.0, ((0, 8), (2, 32)))
    amplitudes = noise(splits[4], (NOCC, NVIRT), NVIRT ** -0.5, 0.125, ((1, 32),))
    return {"chol_vv": chol_vv, "chol_ov": chol_ov, "chol_oo": chol_oo, "chol_vo": chol_vo, "amplitudes": amplitudes}


def reference(chol_vv, chol_ov, chol_oo, chol_vo, amplitudes):
    def one_vector(blocks):
        block_vv, block_ov, block_oo, block_vo = blocks
        lprime = (block_oo.astype(jnp.float32) + jnp.dot(block_ov, amplitudes.T, preferred_element_type=jnp.float32)).astype(jnp.bfloat16)
        direct = jnp.dot(amplitudes, block_vv.T, preferred_element_type=jnp.float32)
        occupied = jnp.dot(lprime.T, amplitudes, preferred_element_type=jnp.float32)
        return (block_vo.astype(jnp.float32) + direct - occupied).astype(jnp.bfloat16)

    dressed = lax.map(one_vector, (chol_vv, chol_ov, chol_oo, chol_vo))
    amps_wide = amplitudes.astype(jnp.float32)

    def one_coulomb(block):
        return 2.0 * jnp.sum(block.astype(jnp.float32) * amps_wide)

    coulomb = lax.map(one_coulomb, dressed)

    def add_vector(total, item):
        weight, block = item
        return total + weight * block.astype(jnp.float32), None

    start = jnp.zeros(amplitudes.shape, jnp.float32)
    total, unused = lax.scan(add_vector, start, (coulomb, dressed))
    fock_ov = total / (QB * N_PB)
    return dressed, fock_ov
```

```python
import jax
import jax.numpy as jnp
from jax import lax
from jax.experimental import pallas as pl
from jax.experimental.pallas import tpu as pltpu
from jax.sharding import PartitionSpec as P

BF, F32 = jnp.bfloat16, jnp.float32
MESH = pl.DeviceIdType.MESH
NZ, NY, NPB = 8, 4, 8
NPQ = NZ * NY
NOCC, NVIRT, QB = 256, 1792, 44
AB, JB = NVIRT // NPQ, NOCC // NPQ
LP_OFF = 672
ROWS = 224
ZORDER = (1, 7, 2, 6, 3, 5, 4)


def dot_t(a, b):
    return lax.dot_general(a, b, (((1,), (1,)), ((), ())), preferred_element_type=F32)


def kernel(vv, ov, oo, vo, am, dressed, fock_out,
           vv_v, ov_v, oo_v, vo_v, t_own, slots, tmat, dbuf, send_a, send_b, recv_a, recv_b,
           lp, occ, dr, fock, fock_r, coul_s, coul_r, coul_b, pq,
           lsem, zsend, zrecv, ysend, yrecv, csend, crecv, msend, mrecv, qsend, qrecv, fsend, frecv, osem):
    pb, me = lax.axis_index("pb"), lax.axis_index("pq")
    z, y = me // NY, me % NY
    half = pb % 2
    partner = pb + 1 - 2 * half

    def zpeer(d):
        return lax.rem(z + d, NZ) * NY + y

    def ypeer(d):
        return z * NY + lax.rem(y + d, NY)

    bar = pltpu.get_barrier_semaphore()
    for d in range(1, NZ):
        pl.semaphore_signal(bar, inc=1, device_id=(pb, zpeer(d)), device_id_type=MESH)
    for d in range(1, NY):
        pl.semaphore_signal(bar, inc=1, device_id=(pb, ypeer(d)), device_id_type=MESH)
    for d in range(1, NPB):
        pl.semaphore_signal(bar, inc=1, device_id=(lax.rem(pb + d, NPB), me), device_id_type=MESH)

    own_slot = y * NZ + z
    loads = [
        pltpu.make_async_copy(
            am.at[:, :, pl.ds(pl.multiple_of(128 * half, 128), 128)], slots.at[half, own_slot], lsem.at[0]),
        pltpu.make_async_copy(am, t_own, lsem.at[1]),
        pltpu.make_async_copy(oo, oo_v, lsem.at[2]),
        pltpu.make_async_copy(ov, ov_v, lsem.at[3]),
        pltpu.make_async_copy(vo, vo_v, lsem.at[4]),
        pltpu.make_async_copy(vv, vv_v, lsem.at[5]),
    ]
    for c in loads:
        c.start()
    loads[0].wait()
    pl.semaphore_wait(bar, (NZ - 1) + (NY - 1) + (NPB - 1))

    def z_copy(d):
        return pltpu.make_async_remote_copy(
            src_ref=slots.at[half, own_slot], dst_ref=slots.at[half, own_slot],
            send_sem=zsend, recv_sem=zrecv.at[d - 1], device_id=(pb, zpeer(d)), device_id_type=MESH)

    for d in ZORDER:
        z_copy(d).start()

    def y_copy(slot, d):
        return pltpu.make_async_remote_copy(
            src_ref=slots.at[half, slot], dst_ref=slots.at[half, slot],
            send_sem=ysend, recv_sem=yrecv.at[d - 1], device_id=(pb, ypeer(d)), device_id_type=MESH)

    for d in range(1, NY):
        y_copy(own_slot, d).start()
    for d in ZORDER:
        z_copy(d).wait_recv()
        slot = y * NZ + lax.rem(z + NZ - d, NZ)
        for e in range(1, NY):
            y_copy(slot, e).start()

    def c_copy(e):
        group = pl.ds(lax.rem(y + NY - e, NY) * NZ, NZ)
        return pltpu.make_async_remote_copy(
            src_ref=slots.at[half, group], dst_ref=slots.at[half, group],
            send_sem=csend, recv_sem=crecv.at[e], device_id=(partner, me), device_id_type=MESH)

    c_copy(0).start()

    for e in range(1, NY):
        group = pl.ds(lax.rem(y + NY - e, NY) * NZ, NZ)
        pltpu.make_async_copy(slots.at[half, group], slots.at[half, group], yrecv.at[e - 1]).wait()
        c_copy(e).start()
    for e in range(NY):
        group = pl.ds(lax.rem(y + NY - e, NY) * NZ, NZ)
        pltpu.make_async_copy(slots.at[1 - half, group], slots.at[1 - half, group], crecv.at[e]).wait()

    def widen(u, carry):
        for hh in range(2):
            for k in range(7):
                parts = []
                for g in (2 * k, 2 * k + 1):
                    p = 2 * u + g // 7
                    slot = lax.rem(p, NY) * NZ + p // NY
                    parts.append(slots[hh, slot, g % 7].astype(F32))
                tmat[pl.ds(pl.multiple_of(112 * u + 16 * k, 16), 16), 128 * hh:128 * hh + 128] = (
                    jnp.concatenate(parts, axis=0).astype(BF))
        return carry

    lax.fori_loop(0, NPQ // 2, widen, 0)

    def all_peer(k):
        return lax.rem(z + k // NY, NZ) * NY + lax.rem(y + k % NY, NY)

    def send_chunk(src, dst, c):
        def body(k, carry):
            peer = all_peer(k)
            pltpu.make_async_remote_copy(
                src_ref=src.at[peer], dst_ref=dst.at[me], send_sem=msend.at[c], recv_sem=mrecv.at[c],
                device_id=(pb, peer), device_id_type=MESH).start()
            return carry
        lax.fori_loop(1, NPQ, body, 0)
        dst[me] = src[me]

    for c in loads[1:]:
        c.wait()
    tw = t_own[...].astype(F32).reshape(1, AB // 8, 8, NOCC)

    def direct(row0, steps, q0):
        def body(s, carry):
            base = pl.multiple_of(s * ROWS, ROWS)
            rows = pl.ds(pl.multiple_of(row0 + base, 32), ROWS)
            d = vo_v[rows, :].astype(F32) + jnp.dot(vv_v[rows, :], tmat[...], preferred_element_type=F32)
            dbuf[pl.ds(base, ROWS), :] = d
            w = jnp.sum(d.reshape(ROWS // AB, AB // 8, 8, NOCC) * tw, axis=1)
            pq[pl.ds(q0 + s * (ROWS // AB), ROWS // AB)] = w[:, :, :128] + w[:, :, 128:]
            return carry
        lax.fori_loop(0, steps, body, 0)

    def ship(tiles, store):
        def body(t, carry):
            at = pl.multiple_of(t * 128, 128)
            store(at, dbuf[pl.ds(at, 128), :].T.reshape(NPQ, 8, 128).astype(BF))
            return carry
        lax.fori_loop(0, tiles, body, 0)

    lpr = oo_v[...].astype(F32) + jnp.dot(ov_v[...], tmat[...], preferred_element_type=F32)
    dbuf[LP_OFF:LP_OFF + 352, :] = lpr
    direct(0, 3, 0)

    def store_a(at, v):
        send_a[:, :, pl.ds(at, 128)] = v

    ship(8, store_a)
    send_chunk(send_a, recv_a, 0)
    lpr = dbuf[LP_OFF:LP_OFF + 352, :].astype(BF).astype(F32)

    def rest(c, carry):
        direct(672 + 896 * c, 4, 12 + 16 * c)

        def store_b(at, v):
            send_b[c, :, :, pl.ds(at, 128)] = v

        ship(7, store_b)
        send_chunk(send_b.at[c], recv_b.at[c], 1 + c)
        return carry

    pick = (lax.broadcasted_iota(jnp.int32, (8, NOCC), 1)
            == me * 8 + lax.broadcasted_iota(jnp.int32, (8, NOCC), 0)).astype(BF)
    own_rows = dot_t(pick, tmat[...]).astype(BF)
    gram = jnp.dot(own_rows, tmat[...], preferred_element_type=F32)
    w = lpr.reshape(QB, 8, NOCC) * gram[None]
    w = w[:, :, :128] + w[:, :, 128:]
    lax.fori_loop(0, 2, rest, 0)

    tot = jnp.sum(pq[...] - w, axis=1)
    tot = jnp.sum(tot, axis=1, keepdims=True)
    eye_q = (lax.broadcasted_iota(jnp.int32, (QB, 128), 0)
             == lax.broadcasted_iota(jnp.int32, (QB, 128), 1)).astype(F32)
    coul_s[0] = jnp.sum(eye_q * tot, axis=0, keepdims=True)

    def q_send(k, carry):
        peer = all_peer(k)
        pltpu.make_async_remote_copy(
            src_ref=coul_s.at[0], dst_ref=coul_r.at[me], send_sem=qsend, recv_sem=qrecv,
            device_id=(pb, peer), device_id_type=MESH).start()
        return carry

    lax.fori_loop(1, NPQ, q_send, 0)
    coul_r[me] = coul_s[0]

    lane = lax.broadcasted_iota(jnp.int32, (8, 128), 1)

    def wait_chunk(dst, c):
        part = dst.at[pl.ds(0, NPQ - 1)]
        pltpu.make_async_copy(part, part, mrecv.at[c]).wait()

    wait_chunk(recv_a, 0)

    def lp_row(q, carry):
        start = LP_OFF + 8 * q
        at = pl.multiple_of(start // 128 * 128, 128)
        off = start % 128
        for hh in range(2):
            acc = None
            for g in range(16):
                v = recv_a[16 * hh + g, :, pl.ds(at, 128)].astype(F32)
                v = pltpu.roll(v, lax.rem(8 * g - off + 128, 128), 1)
                acc = v if acc is None else jnp.where(lane >= 8 * g, v, acc)
            lp[pl.ds(pl.multiple_of(q * 8, 8), 8), 128 * hh:128 * hh + 128] = acc
        return carry

    lax.fori_loop(0, QB, lp_row, 0)
    for n in range(7):
        occ[:, 256 * n:256 * n + 256] = dot_t(lp[...].astype(BF), tmat[256 * n:256 * n + 256, :])

    pltpu.make_async_copy(coul_r.at[pl.ds(0, NPQ - 1)], coul_r.at[pl.ds(0, NPQ - 1)], qrecv).wait()
    coul = 2.0 * jnp.sum(coul_r[...].reshape(NPQ, 128), axis=0, keepdims=True)
    coul_b[...] = jnp.broadcast_to(jnp.sum(eye_q * coul, axis=1, keepdims=True), (QB, 128))

    fock[...] = jnp.zeros((8, NVIRT), F32)

    def gather_q(load, ql, q):
        start = AB * ql
        at = pl.multiple_of(start // 128 * 128, 128)
        nxt = pl.multiple_of(lax.min(at + 128, 768), 128)
        off = start % 128
        tiles = [None] * 14
        for p in range(NPQ):
            dst = AB * p
            o, t = dst % 128, dst // 128
            lo, hi = load(p, at), load(p, nxt)
            sh = lax.rem(o - off + 128, 128)
            lo, hi = pltpu.roll(lo, sh, 1), pltpu.roll(hi, sh, 1)
            src_lane = lax.rem(lane + (128 - o), 128) + off
            v = jnp.where(src_lane < 128, lo, hi)
            if tiles[t] is None:
                tiles[t] = v
            else:
                tiles[t] = jnp.where(lane >= o, v, tiles[t])
            if o + AB > 128:
                tiles[t + 1] = v
        cq = coul_b[pl.ds(q, 1), :]
        rows = pl.ds(pl.multiple_of(q * 8, 8), 8)
        for t in range(14):
            sl = slice(128 * t, 128 * t + 128)
            d = (tiles[t] - occ[rows, sl]).astype(BF)
            dr[q, :, sl] = d
            fock[:, sl] += cq * d.astype(F32)

    def do_a(ql, carry):
        gather_q(lambda p, at: recv_a[p, :, pl.ds(at, 128)].astype(F32), ql, ql)
        return carry

    lax.fori_loop(0, 12, do_a, 0)

    def do_b(c, carry):
        wait_chunk(recv_b.at[c], 1 + c)

        def inner(ql, carry2):
            gather_q(lambda p, at: recv_b[c, p, :, pl.ds(at, 128)].astype(F32), ql, 12 + 16 * c + ql)
            return carry2

        lax.fori_loop(0, 16, inner, 0)
        return carry

    lax.fori_loop(0, 2, do_b, 0)

    out = pltpu.make_async_copy(dr, dressed, osem)
    out.start()

    def f_copy(d):
        return pltpu.make_async_remote_copy(
            src_ref=fock, dst_ref=fock_r.at[pb], send_sem=fsend, recv_sem=frecv,
            device_id=(lax.rem(pb + d, NPB), me), device_id_type=MESH)

    for d in range(1, NPB):
        f_copy(d).start()
    fock_r[pb] = fock[...]
    part = fock_r.at[pl.ds(0, NPB - 1)]
    pltpu.make_async_copy(part, part, frecv).wait()
    fock_out[...] = jnp.sum(fock_r[...], axis=0) * (1.0 / (QB * NPB))

    out.wait()
    zs = slots.at[0, pl.ds(0, NZ - 1)]
    pltpu.make_async_copy(zs, zs, zsend).wait()
    ys = slots.at[0, pl.ds(0, NZ * (NY - 1))]
    pltpu.make_async_copy(ys, ys, ysend).wait()
    cs = slots.at[0]
    pltpu.make_async_copy(cs, cs, csend).wait()
    for c, src in ((0, recv_a), (1, recv_b.at[0]), (2, recv_b.at[1])):
        sp = src.at[pl.ds(0, NPQ - 1)]
        pltpu.make_async_copy(sp, sp, msend.at[c]).wait()
    qp = coul_r.at[pl.ds(0, NPQ - 1)]
    pltpu.make_async_copy(qp, qp, qsend).wait()
    pltpu.make_async_copy(part, part, fsend).wait()


def per_device(chol_vv, chol_ov, chol_oo, chol_vo, amplitudes):
    vv = chol_vv.reshape(QB * AB, NVIRT)
    ov = chol_ov.reshape(QB * JB, NVIRT)
    oo = chol_oo.reshape(QB * JB, NOCC)
    vo = chol_vo.transpose(0, 2, 1).reshape(QB * AB, NOCC)
    am = amplitudes.T.reshape(AB // 8, 8, NOCC)
    dma = pltpu.SemaphoreType.DMA
    return pl.pallas_call(
        kernel,
        out_shape=(jax.ShapeDtypeStruct((QB, JB, NVIRT), BF), jax.ShapeDtypeStruct((JB, NVIRT), F32)),
        in_specs=[pl.BlockSpec(memory_space=pl.ANY)] * 5,
        out_specs=(pl.BlockSpec(memory_space=pl.ANY), pl.BlockSpec(memory_space=pltpu.VMEM)),
        scratch_shapes=[
            pltpu.VMEM((QB * AB, NVIRT), BF),
            pltpu.VMEM((QB * JB, NVIRT), BF),
            pltpu.VMEM((QB * JB, NOCC), BF),
            pltpu.VMEM((QB * AB, NOCC), BF),
            pltpu.VMEM((AB // 8, 8, NOCC), BF),
            pltpu.VMEM((2, NPQ, AB // 8, 8, 128), BF),
            pltpu.VMEM((NVIRT, NOCC), BF),
            pltpu.VMEM((1024, NOCC), F32),
            pltpu.VMEM((NPQ, 8, 1024), BF),
            pltpu.VMEM((2, NPQ, 8, 896), BF),
            pltpu.VMEM((NPQ, 8, 1024), BF),
            pltpu.VMEM((2, NPQ, 8, 896), BF),
            pltpu.VMEM((QB * 8, NOCC), F32),
            pltpu.VMEM((QB * 8, NVIRT), F32),
            pltpu.VMEM((QB, JB, NVIRT), BF),
            pltpu.VMEM((JB, NVIRT), F32),
            pltpu.VMEM((NPB, JB, NVIRT), F32),
            pltpu.VMEM((1, 1, 128), F32),
            pltpu.VMEM((NPQ, 1, 128), F32),
            pltpu.VMEM((QB, 128), F32),
            pltpu.VMEM((QB, 8, 128), F32),
            dma((6,)), dma, dma((NZ - 1,)), dma, dma((NY - 1,)), dma, dma((NY,)),
            dma((3,)), dma((3,)), dma, dma, dma, dma, dma,
        ],
        compiler_params=pltpu.CompilerParams(
            collective_id=0, has_side_effects=True, vmem_limit_bytes=60 * 1024 * 1024),
    )(vv, ov, oo, vo, am)


def solution(mesh):
    in_specs = (
        P("pb", "pq", None),
        P("pb", "pq", None),
        P("pb", "pq", None),
        P("pb", None, "pq"),
        P(None, "pq"),
    )
    out_specs = (P("pb", "pq", None), P("pq", None))
    return jax.shard_map(
        per_device, mesh=mesh, in_specs=in_specs, out_specs=out_specs, check_vma=False
    )
```

```python
import jax
import jax.numpy as jnp
from jax import lax
from jax.experimental import pallas as pl
from jax.experimental.pallas import tpu as pltpu
from jax.sharding import PartitionSpec as P

BF, F32 = jnp.bfloat16, jnp.float32
MESH = pl.DeviceIdType.MESH
NZ, NY, NPB = 8, 4, 8
NPQ = NZ * NY
NOCC, NVIRT, QB = 256, 1792, 44
AB, JB = NVIRT // NPQ, NOCC // NPQ
LP_OFF = 672
ROWS = 224
ZORDER = (1, 7, 2, 6, 3, 5, 4)


def dot_t(a, b):
    return lax.dot_general(a, b, (((1,), (1,)), ((), ())), preferred_element_type=F32)


def kernel(vv, ov, oo, vo, am, dressed, fock_out,
           vv_v, ov_v, oo_v, vo_v, t_own, slots, tmat, dbuf, send_a, send_b, recv_a, recv_b,
           lp, occ, coul_s, coul_r, coul_b, pq, f_t, f_s, f_rs, f_row, f_got, f_all, m_s, m_r,
           lsem, zsend, zrecv, ysend, yrecv, csend, crecv, msend, mrecv, qsend, qrecv, fsend, frecv):
    pb, me = lax.axis_index("pb"), lax.axis_index("pq")
    z, y = me // NY, me % NY
    half = pb % 2
    partner = pb + 1 - 2 * half

    def zpeer(d):
        return lax.rem(z + d, NZ) * NY + y

    def ypeer(d):
        return z * NY + lax.rem(y + d, NY)

    bar = pltpu.get_barrier_semaphore()
    for d in range(1, NZ):
        pl.semaphore_signal(bar, inc=1, device_id=(pb, zpeer(d)), device_id_type=MESH)
    for d in range(1, NY):
        pl.semaphore_signal(bar, inc=1, device_id=(pb, ypeer(d)), device_id_type=MESH)
    for d in range(1, NPB):
        pl.semaphore_signal(bar, inc=1, device_id=(lax.rem(pb + d, NPB), me), device_id_type=MESH)

    own_slot = y * NZ + z
    loads = [
        pltpu.make_async_copy(
            am.at[:, :, pl.ds(pl.multiple_of(128 * half, 128), 128)], slots.at[half, own_slot], lsem.at[0]),
        pltpu.make_async_copy(am, t_own, lsem.at[1]),
        pltpu.make_async_copy(oo, oo_v, lsem.at[2]),
        pltpu.make_async_copy(ov, ov_v, lsem.at[3]),
        pltpu.make_async_copy(vo, vo_v, lsem.at[4]),
        pltpu.make_async_copy(vv, vv_v, lsem.at[5]),
    ]
    for c in loads:
        c.start()
    loads[0].wait()
    pl.semaphore_wait(bar, (NZ - 1) + (NY - 1) + (NPB - 1))

    def z_copy(d):
        return pltpu.make_async_remote_copy(
            src_ref=slots.at[half, own_slot], dst_ref=slots.at[half, own_slot],
            send_sem=zsend, recv_sem=zrecv.at[d - 1], device_id=(pb, zpeer(d)), device_id_type=MESH)

    for d in ZORDER:
        z_copy(d).start()

    def y_copy(slot, d):
        return pltpu.make_async_remote_copy(
            src_ref=slots.at[half, slot], dst_ref=slots.at[half, slot],
            send_sem=ysend, recv_sem=yrecv.at[d - 1], device_id=(pb, ypeer(d)), device_id_type=MESH)

    for d in range(1, NY):
        y_copy(own_slot, d).start()
    for d in ZORDER:
        z_copy(d).wait_recv()
        slot = y * NZ + lax.rem(z + NZ - d, NZ)
        for e in range(1, NY):
            y_copy(slot, e).start()

    def c_copy(e):
        group = pl.ds(lax.rem(y + NY - e, NY) * NZ, NZ)
        return pltpu.make_async_remote_copy(
            src_ref=slots.at[half, group], dst_ref=slots.at[half, group],
            send_sem=csend, recv_sem=crecv.at[e], device_id=(partner, me), device_id_type=MESH)

    c_copy(0).start()

    for e in range(1, NY):
        group = pl.ds(lax.rem(y + NY - e, NY) * NZ, NZ)
        pltpu.make_async_copy(slots.at[half, group], slots.at[half, group], yrecv.at[e - 1]).wait()
        c_copy(e).start()
    for e in range(NY):
        group = pl.ds(lax.rem(y + NY - e, NY) * NZ, NZ)
        pltpu.make_async_copy(slots.at[1 - half, group], slots.at[1 - half, group], crecv.at[e]).wait()

    def widen(u, carry):
        for hh in range(2):
            for k in range(7):
                parts = []
                for g in (2 * k, 2 * k + 1):
                    p = 2 * u + g // 7
                    slot = lax.rem(p, NY) * NZ + p // NY
                    parts.append(slots[hh, slot, g % 7].astype(F32))
                tmat[pl.ds(pl.multiple_of(112 * u + 16 * k, 16), 16), 128 * hh:128 * hh + 128] = (
                    jnp.concatenate(parts, axis=0).astype(BF))
        return carry

    lax.fori_loop(0, NPQ // 2, widen, 0)

    def all_peer(k):
        return lax.rem(z + k // NY, NZ) * NY + lax.rem(y + k % NY, NY)

    def send_piece(src, dst, lo, hi, n):
        lanes = pl.ds(lo, hi - lo)

        def body(k, carry):
            peer = all_peer(k)
            pltpu.make_async_remote_copy(
                src_ref=src.at[peer, :, lanes], dst_ref=dst.at[me, :, lanes],
                send_sem=msend.at[n], recv_sem=mrecv.at[n],
                device_id=(pb, peer), device_id_type=MESH).start()
            return carry

        lax.fori_loop(1, NPQ, body, 0)
        dst[me, :, lo:hi] = src[me, :, lo:hi]

    def wait_piece(dst, lo, hi, n, sem):
        part = dst.at[pl.ds(0, NPQ - 1), :, pl.ds(lo, hi - lo)]
        pltpu.make_async_copy(part, part, sem.at[n]).wait()

    for c in loads[1:]:
        c.wait()
    tw = t_own[...].astype(F32).reshape(1, AB // 8, 8, NOCC)

    def direct(row0, at, q0):
        rows = pl.ds(pl.multiple_of(row0, 32), ROWS)
        d = vo_v[rows, :].astype(F32) + jnp.dot(vv_v[rows, :], tmat[...], preferred_element_type=F32)
        dbuf[pl.ds(pl.multiple_of(at, 32), ROWS), :] = d
        vo_v[rows, :] = d.astype(BF)
        w = jnp.sum(d.reshape(ROWS // AB, AB // 8, 8, NOCC) * tw, axis=1)
        pq[pl.ds(q0, ROWS // AB)] = w[:, :, :128] + w[:, :, 128:]

    def ship(lo, hi, store):
        def body(t, carry):
            at = pl.multiple_of(t * 128, 128)
            store(at, dbuf[pl.ds(at, 128), :].T.reshape(NPQ, 8, 128).astype(BF))
            return carry
        lax.fori_loop(lo, hi, body, 0)

    def store_a(at, v):
        send_a[:, :, pl.ds(at, 128)] = v

    lpr = oo_v[...].astype(F32) + jnp.dot(ov_v[...], tmat[...], preferred_element_type=F32)
    dbuf[LP_OFF:LP_OFF + 352, :] = lpr
    direct(448, 448, 8)
    ship(4, 8, store_a)
    send_piece(send_a, recv_a, 512, 1024, 0)
    lpr = dbuf[LP_OFF:LP_OFF + 352, :].astype(BF).astype(F32)
    direct(0, 0, 0)
    direct(224, 224, 4)
    ship(0, 4, store_a)
    send_piece(send_a, recv_a, 0, 512, 1)

    def rest(c, carry):
        def step(s, carry2):
            direct(672 + 896 * c + s * ROWS, s * ROWS, 12 + 16 * c + 4 * s)
            return carry2

        lax.fori_loop(0, 4, step, 0)

        def store_b(at, v):
            send_b[c, :, :, pl.ds(at, 128)] = v

        ship(0, 7, store_b)
        return carry

    lax.fori_loop(0, 2, rest, 0)

    pick = (lax.broadcasted_iota(jnp.int32, (8, NOCC), 1)
            == me * 8 + lax.broadcasted_iota(jnp.int32, (8, NOCC), 0)).astype(BF)
    own_rows = dot_t(pick, tmat[...]).astype(BF)
    gram = jnp.dot(own_rows, tmat[...], preferred_element_type=F32)
    w = lpr.reshape(QB, 8, NOCC) * gram[None]
    w = w[:, :, :128] + w[:, :, 128:]
    tot = jnp.sum(pq[...] - w, axis=1)
    tot = jnp.sum(tot, axis=1, keepdims=True)
    eye_q = (lax.broadcasted_iota(jnp.int32, (QB, 128), 0)
             == lax.broadcasted_iota(jnp.int32, (QB, 128), 1)).astype(F32)
    coul_s[0] = jnp.sum(eye_q * tot, axis=0, keepdims=True)

    def row_sends(src, dst, ssem, rsem):
        def body(k, carry):
            peer = all_peer(k)
            pltpu.make_async_remote_copy(
                src_ref=src(peer), dst_ref=dst.at[me], send_sem=ssem, recv_sem=rsem,
                device_id=(pb, peer), device_id_type=MESH).start()
            return carry
        lax.fori_loop(1, NPQ, body, 0)

    row_sends(lambda peer: coul_s.at[0], coul_r, qsend, qrecv)
    coul_r[me] = coul_s[0]
    send_piece(send_b.at[0], recv_b.at[0], 0, 896, 2)

    rows_31 = coul_r.at[pl.ds(0, NPQ - 1)]
    pltpu.make_async_copy(rows_31, rows_31, qrecv).wait()
    coul = 2.0 * jnp.sum(coul_r[...].reshape(NPQ, 128), axis=0, keepdims=True)
    coul_b[...] = jnp.broadcast_to(jnp.sum(eye_q * coul, axis=1, keepdims=True), (QB, 128))

    def cq2(q):
        row = coul_b[pl.ds(q, 1), :]
        return jnp.concatenate([row, row], axis=1)

    def f_add(u, acc):
        x = vo_v[pl.ds(pl.multiple_of(u * 2 * AB, 16), 2 * AB), :].astype(F32)
        return acc + cq2(2 * u) * x[:AB] + cq2(2 * u + 1) * x[AB:]

    acc = lax.fori_loop(0, QB // 2, f_add, jnp.zeros((AB, NOCC), F32))
    f_t[...] = jnp.concatenate([acc, jnp.zeros((128 - AB, NOCC), F32)], axis=0).T
    for r in range(8):
        f_s[r] = f_t[pl.ds(r, NPQ, stride=8), :]

    def pb_sends(src, dst, n):
        for d in range(1, NPB):
            to = lax.rem(pb + d, NPB)
            pltpu.make_async_remote_copy(
                src_ref=src(to), dst_ref=dst.at[pb], send_sem=fsend.at[n], recv_sem=frecv.at[n],
                device_id=(to, me), device_id_type=MESH).start()

    def pb_wait(dst, n, sem):
        part = dst.at[pl.ds(0, NPB - 1)]
        pltpu.make_async_copy(part, part, sem.at[n]).wait()

    pb_sends(lambda to: f_s.at[to], f_rs, 0)
    f_rs[pb] = f_s[pb]

    lane = lax.broadcasted_iota(jnp.int32, (8, 128), 1)

    wait_piece(recv_a, 512, 1024, 0, mrecv)

    def lp_row(q, carry):
        start = LP_OFF + 8 * q
        at = pl.multiple_of(start // 128 * 128, 128)
        off = start % 128
        for hh in range(2):
            acc = None
            for g in range(16):
                v = recv_a[16 * hh + g, :, pl.ds(at, 128)].astype(F32)
                v = pltpu.roll(v, lax.rem(8 * g - off + 128, 128), 1)
                acc = v if acc is None else jnp.where(lane >= 8 * g, v, acc)
            lp[pl.ds(pl.multiple_of(q * 8, 8), 8), 128 * hh:128 * hh + 128] = acc
        return carry

    lax.fori_loop(0, QB, lp_row, 0)

    def m_add(q, acc):
        return acc + cq2(q) * lp[pl.ds(pl.multiple_of(q * 8, 8), 8), :]

    m_s[...] = lax.fori_loop(0, QB, m_add, jnp.zeros((8, NOCC), F32))
    pb_sends(lambda to: m_s, m_r, 1)
    m_r[pb] = m_s[...]

    pb_wait(f_rs, 0, frecv)
    tot_f = jnp.sum(f_rs[...], axis=0)
    f_row[...] = tot_f.reshape(NPQ, 1, 128)
    row_sends(lambda peer: f_row.at[peer], f_got, fsend.at[2], frecv.at[2])
    f_got[me] = f_row[me]
    send_piece(send_b.at[1], recv_b.at[1], 0, 640, 3)
    send_piece(send_b.at[1], recv_b.at[1], 640, 896, 4)

    for n in range(7):
        occ[:, 256 * n:256 * n + 256] = dot_t(lp[...].astype(BF), tmat[256 * n:256 * n + 256, :])

    def gather_q(load, ql, q, last):
        start = AB * ql
        at = pl.multiple_of(start // 128 * 128, 128)
        nxt = pl.multiple_of(lax.min(at + 128, last), 128)
        off = start % 128
        tiles = [None] * 14
        for p in range(NPQ):
            dst = AB * p
            o, t = dst % 128, dst // 128
            lo, hi = load(p, at), load(p, nxt)
            sh = lax.rem(o - off + 128, 128)
            lo, hi = pltpu.roll(lo, sh, 1), pltpu.roll(hi, sh, 1)
            src_lane = lax.rem(lane + (128 - o), 128) + off
            v = jnp.where(src_lane < 128, lo, hi)
            if tiles[t] is None:
                tiles[t] = v
            else:
                tiles[t] = jnp.where(lane >= o, v, tiles[t])
            if o + AB > 128:
                tiles[t + 1] = v
        rows = pl.ds(pl.multiple_of(q * 8, 8), 8)
        for t in range(14):
            sl = slice(128 * t, 128 * t + 128)
            dressed[q, :, sl] = (tiles[t] - occ[rows, sl]).astype(BF)

    def do_a(ql, carry):
        gather_q(lambda p, at: recv_a[p, :, pl.ds(at, 128)].astype(F32), ql, ql, 768)
        return carry

    wait_piece(recv_a, 0, 512, 1, mrecv)
    lax.fori_loop(0, 12, do_a, 0)

    def do_b(c, last):
        def inner(ql, carry):
            gather_q(lambda p, at: recv_b[c, p, :, pl.ds(at, 128)].astype(F32), ql, 12 + 16 * c + ql, last)
            return carry
        return inner

    wait_piece(recv_b.at[0], 0, 896, 2, mrecv)
    lax.fori_loop(0, 16, do_b(0, 768), 0)

    got_31 = f_got.at[pl.ds(0, NPQ - 1)]
    pltpu.make_async_copy(got_31, got_31, frecv.at[2]).wait()
    pb_sends(lambda to: f_got, f_all, 3)
    f_all[pb] = f_got[...]
    pb_wait(m_r, 1, frecv)
    m = jnp.sum(m_r[...], axis=0)
    m_hi = m.astype(BF)
    m_lo = m - m_hi.astype(F32)
    m_mid = m_lo.astype(BF)
    m_low = (m_lo - m_mid.astype(F32)).astype(BF)
    f_occ = dot_t(m_hi, tmat[...]) + (dot_t(m_mid, tmat[...]) + dot_t(m_low, tmat[...]))
    pb_wait(f_all, 3, frecv)
    ftiles = [None] * 14
    for p in range(NPQ):
        o, t = AB * p % 128, AB * p // 128
        v = f_all[:, p].reshape(NPB, 128)
        if o:
            v = pltpu.roll(v, o, 1)
        ftiles[t] = v if ftiles[t] is None else jnp.where(lane >= o, v, ftiles[t])
        if o + AB > 128:
            ftiles[t + 1] = v
    for t in range(14):
        sl = slice(128 * t, 128 * t + 128)
        fock_out[:, sl] = (ftiles[t] - f_occ[:, sl]) * (1.0 / (QB * NPB))

    wait_piece(recv_b.at[1], 0, 640, 3, mrecv)
    lax.fori_loop(0, 11, do_b(1, 512), 0)
    wait_piece(recv_b.at[1], 640, 896, 4, mrecv)
    lax.fori_loop(11, 16, do_b(1, 768), 0)

    zs = slots.at[0, pl.ds(0, NZ - 1)]
    pltpu.make_async_copy(zs, zs, zsend).wait()
    ys = slots.at[0, pl.ds(0, NZ * (NY - 1))]
    pltpu.make_async_copy(ys, ys, ysend).wait()
    cs = slots.at[0]
    pltpu.make_async_copy(cs, cs, csend).wait()
    wait_piece(recv_a, 512, 1024, 0, msend)
    wait_piece(recv_a, 0, 512, 1, msend)
    wait_piece(recv_b.at[0], 0, 896, 2, msend)
    wait_piece(recv_b.at[1], 0, 640, 3, msend)
    wait_piece(recv_b.at[1], 640, 896, 4, msend)
    pltpu.make_async_copy(rows_31, rows_31, qsend).wait()
    pltpu.make_async_copy(got_31, got_31, fsend.at[2]).wait()
    pb_wait(f_rs, 0, fsend)
    pb_wait(m_r, 1, fsend)
    pb_wait(f_all, 3, fsend)


def per_device(chol_vv, chol_ov, chol_oo, chol_vo, amplitudes):
    vv = chol_vv.reshape(QB * AB, NVIRT)
    ov = chol_ov.reshape(QB * JB, NVIRT)
    oo = chol_oo.reshape(QB * JB, NOCC)
    vo = chol_vo.transpose(0, 2, 1).reshape(QB * AB, NOCC)
    am = amplitudes.T.reshape(AB // 8, 8, NOCC)
    dma = pltpu.SemaphoreType.DMA
    vv, ov, oo, vo, am = (pltpu.with_memory_space_constraint(x, pltpu.HBM) for x in (vv, ov, oo, vo, am))
    return pl.pallas_call(
        kernel,
        out_shape=(jax.ShapeDtypeStruct((QB, JB, NVIRT), BF), jax.ShapeDtypeStruct((JB, NVIRT), F32)),
        in_specs=[pl.BlockSpec(memory_space=pltpu.HBM)] * 5,
        out_specs=[pl.BlockSpec(memory_space=pltpu.VMEM)] * 2,
        scratch_shapes=[
            pltpu.VMEM((QB * AB, NVIRT), BF),
            pltpu.VMEM((QB * JB, NVIRT), BF),
            pltpu.VMEM((QB * JB, NOCC), BF),
            pltpu.VMEM((QB * AB, NOCC), BF),
            pltpu.VMEM((AB // 8, 8, NOCC), BF),
            pltpu.VMEM((2, NPQ, AB // 8, 8, 128), BF),
            pltpu.VMEM((NVIRT, NOCC), BF),
            pltpu.VMEM((1024, NOCC), F32),
            pltpu.VMEM((NPQ, 8, 1024), BF),
            pltpu.VMEM((2, NPQ, 8, 896), BF),
            pltpu.VMEM((NPQ, 8, 1024), BF),
            pltpu.VMEM((2, NPQ, 8, 896), BF),
            pltpu.VMEM((QB * 8, NOCC), F32),
            pltpu.VMEM((QB * 8, NVIRT), F32),
            pltpu.VMEM((1, 1, 128), F32),
            pltpu.VMEM((NPQ, 1, 128), F32),
            pltpu.VMEM((QB, 128), F32),
            pltpu.VMEM((QB, 8, 128), F32),
            pltpu.VMEM((NOCC, 128), F32),
            pltpu.VMEM((NPB, NPQ, 128), F32),
            pltpu.VMEM((NPB, NPQ, 128), F32),
            pltpu.VMEM((NPQ, 1, 128), F32),
            pltpu.VMEM((NPQ, 1, 128), F32),
            pltpu.VMEM((NPB, NPQ, 1, 128), F32),
            pltpu.VMEM((JB, NOCC), F32),
            pltpu.VMEM((NPB, JB, NOCC), F32),
            dma((6,)), dma, dma((NZ - 1,)), dma, dma((NY - 1,)), dma, dma((NY,)),
            dma((5,)), dma((5,)), dma, dma, dma((4,)), dma((4,)),
        ],
        compiler_params=pltpu.CompilerParams(
            collective_id=0, has_side_effects=True, vmem_limit_bytes=34 * 1024 * 1024),
    )(vv, ov, oo, vo, am)


def solution(mesh):
    in_specs = (
        P("pb", "pq", None),
        P("pb", "pq", None),
        P("pb", "pq", None),
        P("pb", None, "pq"),
        P(None, "pq"),
    )
    out_specs = (P("pb", "pq", None), P("pq", None))
    return jax.shard_map(
        per_device, mesh=mesh, in_specs=in_specs, out_specs=out_specs, check_vma=False
    )
```

```python
import jax
import jax.numpy as jnp
from jax import lax
from jax.experimental import pallas as pl
from jax.experimental.pallas import tpu as pltpu
from jax.sharding import PartitionSpec as P

BF, F32 = jnp.bfloat16, jnp.float32
MESH = pl.DeviceIdType.MESH
NZ, NY, NPB = 8, 4, 8
NPQ = NZ * NY
NOCC, NVIRT, QB = 256, 1792, 44
AB, JB = NVIRT // NPQ, NOCC // NPQ
LP_OFF = 672
ZORDER = (1, 7, 2, 6, 3, 5, 4)


def position(d):
    z, y = d // NY, d % NY
    return (y % 2) * 16 + z * 2 + y // 2


def owner(k):
    return (k % 16) // 2 * NY + k % 2 * 2 + k // 16


def place_matrix():
    a = lax.broadcasted_iota(jnp.int32, (NOCC, NOCC), 0)
    b = lax.broadcasted_iota(jnp.int32, (NOCC, NOCC), 1)
    d = a // 8
    to = (d % 2) * 16 + d // NY * 2 + d % NY // 2
    return (b == to * 8 + a % 8).astype(BF)


def dot_t(a, b):
    return lax.dot_general(a, b, (((1,), (1,)), ((), ())), preferred_element_type=F32)


def kernel(vv, ov, oo, vo, am, dressed, fock_out,
           vv_v, ov_v, oo_v, vo_v, am_v, t_own, slots, tmat, lp_own, send_a, send_b, recv_a, recv_b,
           lp, occ, coul_s, coul_r, coul_b, pq, f_t, f_s, f_rs, f_row, f_got, f_all, m_s, m_r,
           lsem, zsend, zrecv, ysend, yrecv, csend, crecv, msend, mrecv, qsend, qrecv, fsend, frecv):
    pb, me = lax.axis_index("pb"), lax.axis_index("pq")
    z, y = me // NY, me % NY
    half = pb % 2
    partner = pb + 1 - 2 * half

    def zpeer(d):
        return lax.rem(z + d, NZ) * NY + y

    def ypeer(d):
        return z * NY + lax.rem(y + d, NY)

    bar = pltpu.get_barrier_semaphore()
    for d in range(1, NZ):
        pl.semaphore_signal(bar, inc=1, device_id=(pb, zpeer(d)), device_id_type=MESH)
    for d in range(1, NY):
        pl.semaphore_signal(bar, inc=1, device_id=(pb, ypeer(d)), device_id_type=MESH)
    for d in range(1, NPB):
        pl.semaphore_signal(bar, inc=1, device_id=(lax.rem(pb + d, NPB), me), device_id_type=MESH)

    own_slot = y * NZ + z
    loads = [
        pltpu.make_async_copy(am, am_v, lsem.at[0]),
        pltpu.make_async_copy(oo, oo_v, lsem.at[1]),
        pltpu.make_async_copy(ov, ov_v, lsem.at[2]),
        pltpu.make_async_copy(vo, vo_v, lsem.at[3]),
        pltpu.make_async_copy(vv, vv_v, lsem.at[4]),
    ]
    for c in loads:
        c.start()
    loads[0].wait()
    shuffle = place_matrix()
    own = jnp.dot(am_v[...], shuffle, preferred_element_type=F32)
    for k in range(AB // 8):
        t_own[k] = own[8 * k:8 * k + 8].astype(BF)
        for hh in range(2):
            @pl.when(half == hh)
            def _():
                slots[hh, own_slot, k] = own[8 * k:8 * k + 8, 128 * hh:128 * hh + 128].astype(BF)
    loads[1].wait()
    oo_v[...] = jnp.dot(oo_v[...], shuffle, preferred_element_type=F32).astype(BF)
    loads[3].wait()

    def shuffle_vo(c, carry):
        rows = pl.ds(pl.multiple_of(c * 352, 32), 352)
        vo_v[rows, :] = jnp.dot(vo_v[rows, :], shuffle, preferred_element_type=F32).astype(BF)
        return carry

    lax.fori_loop(0, 7, shuffle_vo, 0)
    pl.semaphore_wait(bar, (NZ - 1) + (NY - 1) + (NPB - 1))

    def z_copy(d):
        return pltpu.make_async_remote_copy(
            src_ref=slots.at[half, own_slot], dst_ref=slots.at[half, own_slot],
            send_sem=zsend, recv_sem=zrecv.at[d - 1], device_id=(pb, zpeer(d)), device_id_type=MESH)

    for d in ZORDER:
        z_copy(d).start()

    def y_copy(slot, d):
        return pltpu.make_async_remote_copy(
            src_ref=slots.at[half, slot], dst_ref=slots.at[half, slot],
            send_sem=ysend, recv_sem=yrecv.at[d - 1], device_id=(pb, ypeer(d)), device_id_type=MESH)

    for d in range(1, NY):
        y_copy(own_slot, d).start()
    for d in ZORDER:
        z_copy(d).wait_recv()
        slot = y * NZ + lax.rem(z + NZ - d, NZ)
        for e in range(1, NY):
            y_copy(slot, e).start()

    def c_copy(e):
        group = pl.ds(lax.rem(y + NY - e, NY) * NZ, NZ)
        return pltpu.make_async_remote_copy(
            src_ref=slots.at[half, group], dst_ref=slots.at[half, group],
            send_sem=csend, recv_sem=crecv.at[e], device_id=(partner, me), device_id_type=MESH)

    c_copy(0).start()

    for e in range(1, NY):
        group = pl.ds(lax.rem(y + NY - e, NY) * NZ, NZ)
        pltpu.make_async_copy(slots.at[half, group], slots.at[half, group], yrecv.at[e - 1]).wait()
        c_copy(e).start()
    def widen(hh):
        cols = pl.ds(pl.multiple_of(128 * hh, 128), 128)

        def body(u, carry):
            for k in range(7):
                parts = []
                for g in (2 * k, 2 * k + 1):
                    p = 2 * u + g // 7
                    slot = lax.rem(p, NY) * NZ + p // NY
                    parts.append(slots[hh, slot, g % 7].astype(F32))
                tmat[pl.ds(pl.multiple_of(112 * u + 16 * k, 16), 16), cols] = (
                    jnp.concatenate(parts, axis=0).astype(BF))
            return carry

        lax.fori_loop(0, NPQ // 2, body, 0)

    widen(half)

    def all_peer(k):
        return lax.rem(z + k // NY, NZ) * NY + lax.rem(y + k % NY, NY)

    def send_piece(src, dst, lo, hi, n):
        lanes = pl.ds(lo, hi - lo)

        def body(k, carry):
            peer = all_peer(k)
            pltpu.make_async_remote_copy(
                src_ref=src.at[position(peer), :, lanes], dst_ref=dst.at[me, :, lanes],
                send_sem=msend.at[n], recv_sem=mrecv.at[n],
                device_id=(pb, peer), device_id_type=MESH).start()
            return carry

        lax.fori_loop(1, NPQ, body, 0)
        dst[me, :, lo:hi] = src[position(me), :, lo:hi]

    def send_half(src, dst, lo, hi, n, hh):
        lanes = pl.ds(lo, hi - lo)

        def body(k, carry):
            peer = all_peer(2 * k + lax.rem(y + hh, 2))

            @pl.when(peer != me)
            def _():
                pltpu.make_async_remote_copy(
                    src_ref=src.at[position(peer), :, lanes], dst_ref=dst.at[me, :, lanes],
                    send_sem=msend.at[n], recv_sem=mrecv.at[n],
                    device_id=(pb, peer), device_id_type=MESH).start()
            return carry

        lax.fori_loop(0, 16, body, 0)

    def wait_piece(dst, lo, hi, n, sem):
        part = dst.at[pl.ds(0, NPQ - 1), :, pl.ds(lo, hi - lo)]
        pltpu.make_async_copy(part, part, sem.at[n]).wait()

    loads[2].wait()
    loads[4].wait()
    def direct(row0, n, q0, cols, old=None):
        rows = pl.ds(pl.multiple_of(row0, 32), n)
        d = vo_v[rows, cols].astype(F32) + jnp.dot(vv_v[rows, :], tmat[:, cols], preferred_element_type=F32)
        vo_v[rows, cols] = d.astype(BF)
        w = jnp.sum(d.reshape(n // AB, AB // 8, 8, d.shape[1]) * t_own[:, :, cols].astype(F32)[None], axis=1)
        if d.shape[1] == NOCC:
            w = w[:, :, :128] + w[:, :, 128:]
        here = pl.ds(q0, n // AB)
        pq[here] = w if old is None else pq[here] + w

    def first_chunk(hh, old):
        cols = pl.ds(pl.multiple_of(128 * hh, 128), 128)
        owners = pl.ds(16 * hh, 16)

        def ship(at, block):
            send_a[owners, :, pl.ds(at, 128)] = block.astype(F32).T.reshape(16, 8, 128).astype(BF)

        lp_own[:, cols] = (oo_v[:, cols].astype(F32) + jnp.dot(
            ov_v[...], tmat[:, cols], preferred_element_type=F32)).astype(BF)
        direct(448, 224, 8, cols, old)
        ship(512, vo_v[512:640, cols])
        ship(640, jnp.concatenate([vo_v[640:672, cols], lp_own[0:96, cols]], axis=0))
        ship(768, lp_own[96:224, cols])
        ship(896, lp_own[224:352, cols])
        if old is None:
            send_half(send_a, recv_a, 512, 1024, 0, hh)
        direct(0, 448, 0, cols, old)
        for t in range(4):
            ship(128 * t, vo_v[128 * t:128 * t + 128, cols])
        if old is None:
            send_half(send_a, recv_a, 0, 512, 1, hh)

    first_chunk(half, None)
    for e in range(NY):
        group = pl.ds(lax.rem(y + NY - e, NY) * NZ, NZ)
        pltpu.make_async_copy(slots.at[1 - half, group], slots.at[1 - half, group], crecv.at[e]).wait()
    widen(1 - half)
    first_chunk(1 - half, True)
    recv_a[me] = send_a[position(me)]
    lpr = lp_own[...].astype(F32)

    def rest(c, carry):
        direct(672 + 448 * c, 448, 12 + 8 * c, slice(0, NOCC))
        return carry

    lax.fori_loop(0, 4, rest, 0)

    pick = (lax.broadcasted_iota(jnp.int32, (8, NOCC), 1)
            == position(me) * 8 + lax.broadcasted_iota(jnp.int32, (8, NOCC), 0)).astype(BF)
    own_rows = dot_t(pick, tmat[...]).astype(BF)
    gram = jnp.dot(own_rows, tmat[...], preferred_element_type=F32)
    w = lpr.reshape(QB, 8, NOCC) * gram[None]
    w = w[:, :, :128] + w[:, :, 128:]
    tot = jnp.sum(pq[...] - w, axis=1)
    tot = jnp.sum(tot, axis=1, keepdims=True)
    eye_q = (lax.broadcasted_iota(jnp.int32, (QB, 128), 0)
             == lax.broadcasted_iota(jnp.int32, (QB, 128), 1)).astype(F32)
    coul_s[0] = jnp.sum(eye_q * tot, axis=0, keepdims=True)

    def row_sends(src, dst, ssem, rsem):
        def body(k, carry):
            peer = all_peer(k)
            pltpu.make_async_remote_copy(
                src_ref=src(peer), dst_ref=dst.at[me], send_sem=ssem, recv_sem=rsem,
                device_id=(pb, peer), device_id_type=MESH).start()
            return carry
        lax.fori_loop(1, NPQ, body, 0)

    row_sends(lambda peer: coul_s.at[0], coul_r, qsend, qrecv)
    coul_r[me] = coul_s[0]
    send_half(send_a, recv_a, 512, 1024, 0, 1 - half)
    send_half(send_a, recv_a, 0, 512, 1, 1 - half)

    def ship_b(c):
        def body(t, carry):
            at = pl.multiple_of(t * 128, 128)
            block = vo_v[pl.ds(pl.multiple_of(672 + 896 * c + at, 32), 128), :].astype(F32)
            send_b[c, :, :, pl.ds(at, 128)] = block.T.reshape(NPQ, 8, 128).astype(BF)
            return carry
        lax.fori_loop(0, 7, body, 0)

    ship_b(0)
    ship_b(1)

    rows_31 = coul_r.at[pl.ds(0, NPQ - 1)]
    pltpu.make_async_copy(rows_31, rows_31, qrecv).wait()
    send_piece(send_b.at[0], recv_b.at[0], 0, 896, 2)
    coul = 2.0 * jnp.sum(coul_r[...].reshape(NPQ, 128), axis=0, keepdims=True)
    coul_b[...] = jnp.broadcast_to(jnp.sum(eye_q * coul, axis=1, keepdims=True), (QB, 128))

    def cq2(q):
        row = coul_b[pl.ds(q, 1), :]
        return jnp.concatenate([row, row], axis=1)

    def f_add(u, acc):
        x = vo_v[pl.ds(pl.multiple_of(u * 2 * AB, 16), 2 * AB), :].astype(F32)
        return acc + cq2(2 * u) * x[:AB] + cq2(2 * u + 1) * x[AB:]

    acc = lax.fori_loop(0, QB // 2, f_add, jnp.zeros((AB, NOCC), F32))
    f_t[...] = jnp.concatenate([acc, jnp.zeros((128 - AB, NOCC), F32)], axis=0).T
    for r in range(8):
        f_s[r] = f_t[pl.ds(r, NPQ, stride=8), :]

    def pb_sends(src, dst, n):
        for d in range(1, NPB):
            to = lax.rem(pb + d, NPB)
            pltpu.make_async_remote_copy(
                src_ref=src(to), dst_ref=dst.at[pb], send_sem=fsend.at[n], recv_sem=frecv.at[n],
                device_id=(to, me), device_id_type=MESH).start()

    def pb_wait(dst, n, sem):
        part = dst.at[pl.ds(0, NPB - 1)]
        pltpu.make_async_copy(part, part, sem.at[n]).wait()

    pb_sends(lambda to: f_s.at[to], f_rs, 0)
    f_rs[pb] = f_s[pb]

    lane = lax.broadcasted_iota(jnp.int32, (8, 128), 1)

    wait_piece(recv_a, 512, 1024, 0, mrecv)

    def lp_row(q, carry):
        start = LP_OFF + 8 * q
        at = pl.multiple_of(start // 128 * 128, 128)
        off = start % 128
        for hh in range(2):
            acc = None
            for g in range(16):
                v = recv_a[owner(16 * hh + g), :, pl.ds(at, 128)].astype(F32)
                v = pltpu.roll(v, lax.rem(8 * g - off + 128, 128), 1)
                acc = v if acc is None else jnp.where(lane >= 8 * g, v, acc)
            lp[pl.ds(pl.multiple_of(q * 8, 8), 8), 128 * hh:128 * hh + 128] = acc
        return carry

    lax.fori_loop(0, QB, lp_row, 0)

    def m_add(q, acc):
        return acc + cq2(q) * lp[pl.ds(pl.multiple_of(q * 8, 8), 8), :]

    m_s[...] = lax.fori_loop(0, QB, m_add, jnp.zeros((8, NOCC), F32))
    pb_sends(lambda to: m_s, m_r, 1)
    m_r[pb] = m_s[...]

    pb_wait(f_rs, 0, frecv)
    tot_f = jnp.sum(f_rs[...], axis=0)
    f_row[...] = tot_f.reshape(NPQ, 1, 128)
    row_sends(lambda peer: f_row.at[position(peer)], f_got, fsend.at[2], frecv.at[2])
    f_got[me] = f_row[position(me)]
    send_piece(send_b.at[1], recv_b.at[1], 0, 640, 3)
    send_piece(send_b.at[1], recv_b.at[1], 640, 896, 4)

    for n in range(7):
        occ[:, 256 * n:256 * n + 256] = dot_t(lp[...].astype(BF), tmat[256 * n:256 * n + 256, :])

    def gather_q(load, ql, q, last):
        start = AB * ql
        at = pl.multiple_of(start // 128 * 128, 128)
        nxt = pl.multiple_of(lax.min(at + 128, last), 128)
        off = start % 128
        tiles = [None] * 14
        for p in range(NPQ):
            dst = AB * p
            o, t = dst % 128, dst // 128
            lo, hi = load(p, at), load(p, nxt)
            sh = lax.rem(o - off + 128, 128)
            lo, hi = pltpu.roll(lo, sh, 1), pltpu.roll(hi, sh, 1)
            src_lane = lax.rem(lane + (128 - o), 128) + off
            v = jnp.where(src_lane < 128, lo, hi)
            if tiles[t] is None:
                tiles[t] = v
            else:
                tiles[t] = jnp.where(lane >= o, v, tiles[t])
            if o + AB > 128:
                tiles[t + 1] = v
        rows = pl.ds(pl.multiple_of(q * 8, 8), 8)
        for t in range(14):
            sl = slice(128 * t, 128 * t + 128)
            dressed[q, :, sl] = (tiles[t] - occ[rows, sl]).astype(BF)

    def do_a(ql, carry):
        gather_q(lambda p, at: recv_a[p, :, pl.ds(at, 128)].astype(F32), ql, ql, 768)
        return carry

    wait_piece(recv_a, 0, 512, 1, mrecv)
    lax.fori_loop(0, 12, do_a, 0)

    def do_b(c, last):
        def inner(ql, carry):
            gather_q(lambda p, at: recv_b[c, p, :, pl.ds(at, 128)].astype(F32), ql, 12 + 16 * c + ql, last)
            return carry
        return inner

    wait_piece(recv_b.at[0], 0, 896, 2, mrecv)
    got_31 = f_got.at[pl.ds(0, NPQ - 1)]
    pltpu.make_async_copy(got_31, got_31, frecv.at[2]).wait()
    pb_sends(lambda to: f_got, f_all, 3)
    f_all[pb] = f_got[...]
    lax.fori_loop(0, 16, do_b(0, 768), 0)

    wait_piece(recv_b.at[1], 0, 640, 3, mrecv)
    lax.fori_loop(0, 11, do_b(1, 512), 0)

    pb_wait(m_r, 1, frecv)
    m = jnp.sum(m_r[...], axis=0)
    m_hi = m.astype(BF)
    m_lo = m - m_hi.astype(F32)
    m_mid = m_lo.astype(BF)
    m_low = (m_lo - m_mid.astype(F32)).astype(BF)
    f_occ = dot_t(m_hi, tmat[...]) + (dot_t(m_mid, tmat[...]) + dot_t(m_low, tmat[...]))
    pb_wait(f_all, 3, frecv)
    ftiles = [None] * 14
    for p in range(NPQ):
        o, t = AB * p % 128, AB * p // 128
        v = f_all[:, p].reshape(NPB, 128)
        if o:
            v = pltpu.roll(v, o, 1)
        ftiles[t] = v if ftiles[t] is None else jnp.where(lane >= o, v, ftiles[t])
        if o + AB > 128:
            ftiles[t + 1] = v
    for t in range(14):
        sl = slice(128 * t, 128 * t + 128)
        fock_out[:, sl] = (ftiles[t] - f_occ[:, sl]) * (1.0 / (QB * NPB))

    wait_piece(recv_b.at[1], 640, 896, 4, mrecv)
    lax.fori_loop(11, 16, do_b(1, 768), 0)

    zs = slots.at[0, pl.ds(0, NZ - 1)]
    pltpu.make_async_copy(zs, zs, zsend).wait()
    ys = slots.at[0, pl.ds(0, NZ * (NY - 1))]
    pltpu.make_async_copy(ys, ys, ysend).wait()
    cs = slots.at[0]
    pltpu.make_async_copy(cs, cs, csend).wait()
    wait_piece(recv_a, 512, 1024, 0, msend)
    wait_piece(recv_a, 0, 512, 1, msend)
    wait_piece(recv_b.at[0], 0, 896, 2, msend)
    wait_piece(recv_b.at[1], 0, 640, 3, msend)
    wait_piece(recv_b.at[1], 640, 896, 4, msend)
    pltpu.make_async_copy(rows_31, rows_31, qsend).wait()
    pltpu.make_async_copy(got_31, got_31, fsend.at[2]).wait()
    pb_wait(f_rs, 0, fsend)
    pb_wait(m_r, 1, fsend)
    pb_wait(f_all, 3, fsend)


def per_device(chol_vv, chol_ov, chol_oo, chol_vo, amplitudes):
    vv = chol_vv.reshape(QB * AB, NVIRT)
    ov = chol_ov.reshape(QB * JB, NVIRT)
    oo = chol_oo.reshape(QB * JB, NOCC)
    vo = chol_vo.transpose(0, 2, 1).reshape(QB * AB, NOCC)
    am = amplitudes.T
    dma = pltpu.SemaphoreType.DMA
    vv, ov, oo, vo, am = (pltpu.with_memory_space_constraint(x, pltpu.HBM) for x in (vv, ov, oo, vo, am))
    return pl.pallas_call(
        kernel,
        out_shape=(jax.ShapeDtypeStruct((QB, JB, NVIRT), BF), jax.ShapeDtypeStruct((JB, NVIRT), F32)),
        in_specs=[pl.BlockSpec(memory_space=pltpu.HBM)] * 5,
        out_specs=[pl.BlockSpec(memory_space=pltpu.VMEM)] * 2,
        scratch_shapes=[
            pltpu.VMEM((QB * AB, NVIRT), BF),
            pltpu.VMEM((QB * JB, NVIRT), BF),
            pltpu.VMEM((QB * JB, NOCC), BF),
            pltpu.VMEM((QB * AB, NOCC), BF),
            pltpu.VMEM((AB, NOCC), BF),
            pltpu.VMEM((AB // 8, 8, NOCC), BF),
            pltpu.VMEM((2, NPQ, AB // 8, 8, 128), BF),
            pltpu.VMEM((NVIRT, NOCC), BF),
            pltpu.VMEM((QB * JB, NOCC), BF),
            pltpu.VMEM((NPQ, 8, 1024), BF),
            pltpu.VMEM((2, NPQ, 8, 896), BF),
            pltpu.VMEM((NPQ, 8, 1024), BF),
            pltpu.VMEM((2, NPQ, 8, 896), BF),
            pltpu.VMEM((QB * 8, NOCC), F32),
            pltpu.VMEM((QB * 8, NVIRT), F32),
            pltpu.VMEM((1, 1, 128), F32),
            pltpu.VMEM((NPQ, 1, 128), F32),
            pltpu.VMEM((QB, 128), F32),
            pltpu.VMEM((QB, 8, 128), F32),
            pltpu.VMEM((NOCC, 128), F32),
            pltpu.VMEM((NPB, NPQ, 128), F32),
            pltpu.VMEM((NPB, NPQ, 128), F32),
            pltpu.VMEM((NPQ, 1, 128), F32),
            pltpu.VMEM((NPQ, 1, 128), F32),
            pltpu.VMEM((NPB, NPQ, 1, 128), F32),
            pltpu.VMEM((JB, NOCC), F32),
            pltpu.VMEM((NPB, JB, NOCC), F32),
            dma((5,)), dma, dma((NZ - 1,)), dma, dma((NY - 1,)), dma, dma((NY,)),
            dma((5,)), dma((5,)), dma, dma, dma((4,)), dma((4,)),
        ],
        compiler_params=pltpu.CompilerParams(
            collective_id=0, has_side_effects=True, vmem_limit_bytes=34 * 1024 * 1024),
    )(vv, ov, oo, vo, am)


def solution(mesh):
    in_specs = (
        P("pb", "pq", None),
        P("pb", "pq", None),
        P("pb", "pq", None),
        P("pb", None, "pq"),
        P(None, "pq"),
    )
    out_specs = (P("pb", "pq", None), P("pq", None))
    return jax.shard_map(
        per_device, mesh=mesh, in_specs=in_specs, out_specs=out_specs, check_vma=False
    )
```

```python
import jax
import jax.numpy as jnp
from jax import lax
from jax.experimental import pallas as pl
from jax.experimental.pallas import tpu as pltpu
from jax.sharding import PartitionSpec as P

BF, F32 = jnp.bfloat16, jnp.float32
MESH = pl.DeviceIdType.MESH
NZ, NY, NPB = 8, 4, 8
NPQ = NZ * NY
NOCC, NVIRT, QB = 256, 1792, 44
AB, JB = NVIRT // NPQ, NOCC // NPQ
LP_OFF = 672
ZORDER = (1, 7, 2, 6, 3, 5, 4)


def position(d):
    z, y = d // NY, d % NY
    return (y % 2) * 16 + z * 2 + y // 2


def owner(k):
    return (k % 16) // 2 * NY + k % 2 * 2 + k // 16


def place_matrix():
    a = lax.broadcasted_iota(jnp.int32, (NOCC, NOCC), 0)
    b = lax.broadcasted_iota(jnp.int32, (NOCC, NOCC), 1)
    d = a // 8
    to = (d % 2) * 16 + d // NY * 2 + d % NY // 2
    return (b == to * 8 + a % 8).astype(BF)


def dot_t(a, b):
    return lax.dot_general(a, b, (((1,), (1,)), ((), ())), preferred_element_type=F32)


def kernel(vv, ov, oo, vo, am, dressed, fock_out,
           vv_v, ov_v, oo_v, vo_v, am_v, t_own, slots, tmat, lp_own, send_a, send_b, recv_a, recv_b,
           lp, occ, coul_s, coul_r, coul_b, pq, f_t, f_s, f_rs, f_row, f_got, f_all, m_s, m_r,
           lsem, zsend, zrecv, ysend, yrecv, csend, crecv, msend, mrecv, qsend, qrecv, fsend, frecv):
    pb, me = lax.axis_index("pb"), lax.axis_index("pq")
    z, y = me // NY, me % NY
    half = pb % 2
    partner = pb + 1 - 2 * half

    def zpeer(d):
        return lax.rem(z + d, NZ) * NY + y

    def ypeer(d):
        return z * NY + lax.rem(y + d, NY)

    bar = pltpu.get_barrier_semaphore()
    for d in range(1, NZ):
        pl.semaphore_signal(bar, inc=1, device_id=(pb, zpeer(d)), device_id_type=MESH)
    for d in range(1, NY):
        pl.semaphore_signal(bar, inc=1, device_id=(pb, ypeer(d)), device_id_type=MESH)
    for d in range(1, NPB):
        pl.semaphore_signal(bar, inc=1, device_id=(lax.rem(pb + d, NPB), me), device_id_type=MESH)

    own_slot = y * NZ + z
    loads = [
        pltpu.make_async_copy(am, am_v, lsem.at[0]),
        pltpu.make_async_copy(oo, oo_v, lsem.at[1]),
        pltpu.make_async_copy(ov, ov_v, lsem.at[2]),
        pltpu.make_async_copy(vo, vo_v, lsem.at[3]),
        pltpu.make_async_copy(vv, vv_v, lsem.at[4]),
    ]
    for c in loads:
        c.start()
    loads[0].wait()
    shuffle = place_matrix()
    own = jnp.dot(am_v[...], shuffle, preferred_element_type=F32)
    for k in range(AB // 8):
        t_own[k] = own[8 * k:8 * k + 8].astype(BF)
        for hh in range(2):
            @pl.when(half == hh)
            def _():
                slots[hh, own_slot, k] = own[8 * k:8 * k + 8, 128 * hh:128 * hh + 128].astype(BF)
    loads[1].wait()
    oo_v[...] = jnp.dot(oo_v[...], shuffle, preferred_element_type=F32).astype(BF)
    loads[3].wait()

    def shuffle_vo(c, carry):
        rows = pl.ds(pl.multiple_of(c * 352, 32), 352)
        vo_v[rows, :] = jnp.dot(vo_v[rows, :], shuffle, preferred_element_type=F32).astype(BF)
        return carry

    lax.fori_loop(0, 7, shuffle_vo, 0)
    pl.semaphore_wait(bar, (NZ - 1) + (NY - 1) + (NPB - 1))

    def z_copy(d):
        return pltpu.make_async_remote_copy(
            src_ref=slots.at[half, own_slot], dst_ref=slots.at[half, own_slot],
            send_sem=zsend, recv_sem=zrecv.at[d - 1], device_id=(pb, zpeer(d)), device_id_type=MESH)

    for d in ZORDER:
        z_copy(d).start()

    def y_copy(slot, d):
        return pltpu.make_async_remote_copy(
            src_ref=slots.at[half, slot], dst_ref=slots.at[half, slot],
            send_sem=ysend, recv_sem=yrecv.at[d - 1], device_id=(pb, ypeer(d)), device_id_type=MESH)

    for d in range(1, NY):
        y_copy(own_slot, d).start()
    for d in ZORDER:
        z_copy(d).wait_recv()
        slot = y * NZ + lax.rem(z + NZ - d, NZ)
        for e in range(1, NY):
            y_copy(slot, e).start()

    def c_copy(e):
        group = pl.ds(lax.rem(y + NY - e, NY) * NZ, NZ)
        return pltpu.make_async_remote_copy(
            src_ref=slots.at[half, group], dst_ref=slots.at[half, group],
            send_sem=csend, recv_sem=crecv.at[e], device_id=(partner, me), device_id_type=MESH)

    c_copy(0).start()

    for e in range(1, NY):
        group = pl.ds(lax.rem(y + NY - e, NY) * NZ, NZ)
        pltpu.make_async_copy(slots.at[half, group], slots.at[half, group], yrecv.at[e - 1]).wait()
        c_copy(e).start()
    def widen(hh):
        cols = pl.ds(pl.multiple_of(128 * hh, 128), 128)

        def body(u, carry):
            for k in range(7):
                parts = []
                for g in (2 * k, 2 * k + 1):
                    p = 2 * u + g // 7
                    slot = lax.rem(p, NY) * NZ + p // NY
                    parts.append(slots[hh, slot, g % 7].astype(F32))
                tmat[pl.ds(pl.multiple_of(112 * u + 16 * k, 16), 16), cols] = (
                    jnp.concatenate(parts, axis=0).astype(BF))
            return carry

        lax.fori_loop(0, NPQ // 2, body, 0)

    widen(half)

    def all_peer(k):
        return lax.rem(z + k // NY, NZ) * NY + lax.rem(y + k % NY, NY)

    def send_piece(src, dst, lo, hi, n):
        lanes = pl.ds(lo, hi - lo)

        def body(k, carry):
            peer = all_peer(k)
            pltpu.make_async_remote_copy(
                src_ref=src.at[position(peer), :, lanes], dst_ref=dst.at[me, :, lanes],
                send_sem=msend.at[n], recv_sem=mrecv.at[n],
                device_id=(pb, peer), device_id_type=MESH).start()
            return carry

        lax.fori_loop(1, NPQ, body, 0)
        dst[me, :, lo:hi] = src[position(me), :, lo:hi]

    def send_half(src, dst, lo, hi, n, hh):
        lanes = pl.ds(lo, hi - lo)

        def body(k, carry):
            peer = all_peer(2 * k + lax.rem(y + hh, 2))

            @pl.when(peer != me)
            def _():
                pltpu.make_async_remote_copy(
                    src_ref=src.at[position(peer), :, lanes], dst_ref=dst.at[me, :, lanes],
                    send_sem=msend.at[n], recv_sem=mrecv.at[n],
                    device_id=(pb, peer), device_id_type=MESH).start()
            return carry

        lax.fori_loop(0, 16, body, 0)

    def wait_piece(dst, lo, hi, n, sem):
        part = dst.at[pl.ds(0, NPQ - 1), :, pl.ds(lo, hi - lo)]
        pltpu.make_async_copy(part, part, sem.at[n]).wait()

    loads[2].wait()
    loads[4].wait()
    def direct(row0, n, q0, cols, old=None):
        rows = pl.ds(pl.multiple_of(row0, 32), n)
        d = vo_v[rows, cols].astype(F32) + jnp.dot(vv_v[rows, :], tmat[:, cols], preferred_element_type=F32)
        vo_v[rows, cols] = d.astype(BF)
        w = jnp.sum(d.reshape(n // AB, AB // 8, 8, d.shape[1]) * t_own[:, :, cols].astype(F32)[None], axis=1)
        if d.shape[1] == NOCC:
            w = w[:, :, :128] + w[:, :, 128:]
        here = pl.ds(q0, n // AB)
        pq[here] = w if old is None else pq[here] + w

    def first_chunk(hh, old, compute, move):
        cols = pl.ds(pl.multiple_of(128 * hh, 128), 128)
        owners = pl.ds(16 * hh, 16)

        def ship(at, block):
            send_a[owners, :, pl.ds(at, 128)] = block.astype(F32).T.reshape(16, 8, 128).astype(BF)

        if compute:
            lp_own[:, cols] = (oo_v[:, cols].astype(F32) + jnp.dot(
                ov_v[...], tmat[:, cols], preferred_element_type=F32)).astype(BF)
            direct(448, 224, 8, cols, old)
        if move:
            ship(512, vo_v[512:640, cols])
            ship(640, jnp.concatenate([vo_v[640:672, cols], lp_own[0:96, cols]], axis=0))
            ship(768, lp_own[96:224, cols])
            ship(896, lp_own[224:352, cols])
            send_half(send_a, recv_a, 512, 1024, 0, hh)
        if compute:
            direct(0, 448, 0, cols, old)
        if move:
            for t in range(4):
                ship(128 * t, vo_v[128 * t:128 * t + 128, cols])
            send_half(send_a, recv_a, 0, 512, 1, hh)

    first_chunk(half, None, True, True)
    for e in range(NY):
        group = pl.ds(lax.rem(y + NY - e, NY) * NZ, NZ)
        pltpu.make_async_copy(slots.at[1 - half, group], slots.at[1 - half, group], crecv.at[e]).wait()
    widen(1 - half)
    first_chunk(1 - half, True, True, False)
    lpr = lp_own[...].astype(F32)

    def rest(c, carry):
        direct(672 + 448 * c, 448, 12 + 8 * c, slice(0, NOCC))
        return carry

    lax.fori_loop(0, 4, rest, 0)

    pick = (lax.broadcasted_iota(jnp.int32, (8, NOCC), 1)
            == position(me) * 8 + lax.broadcasted_iota(jnp.int32, (8, NOCC), 0)).astype(BF)
    own_rows = dot_t(pick, tmat[...]).astype(BF)
    gram = jnp.dot(own_rows, tmat[...], preferred_element_type=F32)
    w = lpr.reshape(QB, 8, NOCC) * gram[None]
    w = w[:, :, :128] + w[:, :, 128:]
    tot = jnp.sum(pq[...] - w, axis=1)
    tot = jnp.sum(tot, axis=1, keepdims=True)
    eye_q = (lax.broadcasted_iota(jnp.int32, (QB, 128), 0)
             == lax.broadcasted_iota(jnp.int32, (QB, 128), 1)).astype(F32)
    coul_s[0] = jnp.sum(eye_q * tot, axis=0, keepdims=True)

    def row_sends(src, dst, ssem, rsem):
        def body(k, carry):
            peer = all_peer(k)
            pltpu.make_async_remote_copy(
                src_ref=src(peer), dst_ref=dst.at[me], send_sem=ssem, recv_sem=rsem,
                device_id=(pb, peer), device_id_type=MESH).start()
            return carry
        lax.fori_loop(1, NPQ, body, 0)

    row_sends(lambda peer: coul_s.at[0], coul_r, qsend, qrecv)
    coul_r[me] = coul_s[0]
    first_chunk(1 - half, True, False, True)
    recv_a[me] = send_a[position(me)]

    def ship_b(c):
        def body(t, carry):
            at = pl.multiple_of(t * 128, 128)
            block = vo_v[pl.ds(pl.multiple_of(672 + 896 * c + at, 32), 128), :].astype(F32)
            send_b[c, :, :, pl.ds(at, 128)] = block.T.reshape(NPQ, 8, 128).astype(BF)
            return carry
        lax.fori_loop(0, 7, body, 0)

    ship_b(0)
    ship_b(1)

    rows_31 = coul_r.at[pl.ds(0, NPQ - 1)]
    pltpu.make_async_copy(rows_31, rows_31, qrecv).wait()
    send_piece(send_b.at[0], recv_b.at[0], 0, 896, 2)
    coul = 2.0 * jnp.sum(coul_r[...].reshape(NPQ, 128), axis=0, keepdims=True)
    coul_b[...] = jnp.broadcast_to(jnp.sum(eye_q * coul, axis=1, keepdims=True), (QB, 128))

    def cq2(q):
        row = coul_b[pl.ds(q, 1), :]
        return jnp.concatenate([row, row], axis=1)

    def f_add(u, acc):
        x = vo_v[pl.ds(pl.multiple_of(u * 2 * AB, 16), 2 * AB), :].astype(F32)
        return acc + cq2(2 * u) * x[:AB] + cq2(2 * u + 1) * x[AB:]

    acc = lax.fori_loop(0, QB // 2, f_add, jnp.zeros((AB, NOCC), F32))
    f_t[...] = jnp.concatenate([acc, jnp.zeros((128 - AB, NOCC), F32)], axis=0).T
    for r in range(8):
        f_s[r] = f_t[pl.ds(r, NPQ, stride=8), :]

    def pb_sends(src, dst, n):
        for d in range(1, NPB):
            to = lax.rem(pb + d, NPB)
            pltpu.make_async_remote_copy(
                src_ref=src(to), dst_ref=dst.at[pb], send_sem=fsend.at[n], recv_sem=frecv.at[n],
                device_id=(to, me), device_id_type=MESH).start()

    def pb_wait(dst, n, sem):
        part = dst.at[pl.ds(0, NPB - 1)]
        pltpu.make_async_copy(part, part, sem.at[n]).wait()

    pb_sends(lambda to: f_s.at[to], f_rs, 0)
    f_rs[pb] = f_s[pb]

    lane = lax.broadcasted_iota(jnp.int32, (8, 128), 1)

    wait_piece(recv_a, 512, 1024, 0, mrecv)

    def lp_row(q, carry):
        start = LP_OFF + 8 * q
        at = pl.multiple_of(start // 128 * 128, 128)
        off = start % 128
        for hh in range(2):
            acc = None
            for g in range(16):
                v = recv_a[owner(16 * hh + g), :, pl.ds(at, 128)].astype(F32)
                v = pltpu.roll(v, lax.rem(8 * g - off + 128, 128), 1)
                acc = v if acc is None else jnp.where(lane >= 8 * g, v, acc)
            lp[pl.ds(pl.multiple_of(q * 8, 8), 8), 128 * hh:128 * hh + 128] = acc
        return carry

    lax.fori_loop(0, QB, lp_row, 0)

    def m_add(q, acc):
        return acc + cq2(q) * lp[pl.ds(pl.multiple_of(q * 8, 8), 8), :]

    m_s[...] = lax.fori_loop(0, QB, m_add, jnp.zeros((8, NOCC), F32))
    pb_sends(lambda to: m_s, m_r, 1)
    m_r[pb] = m_s[...]

    pb_wait(f_rs, 0, frecv)
    tot_f = jnp.sum(f_rs[...], axis=0)
    f_row[...] = tot_f.reshape(NPQ, 1, 128)
    row_sends(lambda peer: f_row.at[position(peer)], f_got, fsend.at[2], frecv.at[2])
    f_got[me] = f_row[position(me)]
    send_piece(send_b.at[1], recv_b.at[1], 0, 640, 3)
    send_piece(send_b.at[1], recv_b.at[1], 640, 896, 4)

    for n in range(7):
        occ[:, 256 * n:256 * n + 256] = dot_t(lp[...].astype(BF), tmat[256 * n:256 * n + 256, :])

    def gather_q(load, ql, q, last):
        start = AB * ql
        at = pl.multiple_of(start // 128 * 128, 128)
        nxt = pl.multiple_of(lax.min(at + 128, last), 128)
        off = start % 128
        tiles = [None] * 14
        for p in range(NPQ):
            dst = AB * p
            o, t = dst % 128, dst // 128
            lo, hi = load(p, at), load(p, nxt)
            sh = lax.rem(o - off + 128, 128)
            lo, hi = pltpu.roll(lo, sh, 1), pltpu.roll(hi, sh, 1)
            src_lane = lax.rem(lane + (128 - o), 128) + off
            v = jnp.where(src_lane < 128, lo, hi)
            if tiles[t] is None:
                tiles[t] = v
            else:
                tiles[t] = jnp.where(lane >= o, v, tiles[t])
            if o + AB > 128:
                tiles[t + 1] = v
        rows = pl.ds(pl.multiple_of(q * 8, 8), 8)
        for t in range(14):
            sl = slice(128 * t, 128 * t + 128)
            dressed[q, :, sl] = (tiles[t] - occ[rows, sl]).astype(BF)

    def do_a(ql, carry):
        gather_q(lambda p, at: recv_a[p, :, pl.ds(at, 128)].astype(F32), ql, ql, 768)
        return carry

    wait_piece(recv_a, 0, 512, 1, mrecv)
    lax.fori_loop(0, 12, do_a, 0)

    def do_b(c, last):
        def inner(ql, carry):
            gather_q(lambda p, at: recv_b[c, p, :, pl.ds(at, 128)].astype(F32), ql, 12 + 16 * c + ql, last)
            return carry
        return inner

    wait_piece(recv_b.at[0], 0, 896, 2, mrecv)
    got_31 = f_got.at[pl.ds(0, NPQ - 1)]
    pltpu.make_async_copy(got_31, got_31, frecv.at[2]).wait()
    pb_sends(lambda to: f_got, f_all, 3)
    f_all[pb] = f_got[...]
    lax.fori_loop(0, 16, do_b(0, 768), 0)

    wait_piece(recv_b.at[1], 0, 640, 3, mrecv)
    lax.fori_loop(0, 11, do_b(1, 512), 0)

    pb_wait(m_r, 1, frecv)
    m = jnp.sum(m_r[...], axis=0)
    m_hi = m.astype(BF)
    m_lo = m - m_hi.astype(F32)
    m_mid = m_lo.astype(BF)
    m_low = (m_lo - m_mid.astype(F32)).astype(BF)
    f_occ = dot_t(m_hi, tmat[...]) + (dot_t(m_mid, tmat[...]) + dot_t(m_low, tmat[...]))
    pb_wait(f_all, 3, frecv)
    ftiles = [None] * 14
    for p in range(NPQ):
        o, t = AB * p % 128, AB * p // 128
        v = f_all[:, p].reshape(NPB, 128)
        if o:
            v = pltpu.roll(v, o, 1)
        ftiles[t] = v if ftiles[t] is None else jnp.where(lane >= o, v, ftiles[t])
        if o + AB > 128:
            ftiles[t + 1] = v
    for t in range(14):
        sl = slice(128 * t, 128 * t + 128)
        fock_out[:, sl] = (ftiles[t] - f_occ[:, sl]) * (1.0 / (QB * NPB))

    wait_piece(recv_b.at[1], 640, 896, 4, mrecv)
    lax.fori_loop(11, 16, do_b(1, 768), 0)

    zs = slots.at[0, pl.ds(0, NZ - 1)]
    pltpu.make_async_copy(zs, zs, zsend).wait()
    ys = slots.at[0, pl.ds(0, NZ * (NY - 1))]
    pltpu.make_async_copy(ys, ys, ysend).wait()
    cs = slots.at[0]
    pltpu.make_async_copy(cs, cs, csend).wait()
    wait_piece(recv_a, 512, 1024, 0, msend)
    wait_piece(recv_a, 0, 512, 1, msend)
    wait_piece(recv_b.at[0], 0, 896, 2, msend)
    wait_piece(recv_b.at[1], 0, 640, 3, msend)
    wait_piece(recv_b.at[1], 640, 896, 4, msend)
    pltpu.make_async_copy(rows_31, rows_31, qsend).wait()
    pltpu.make_async_copy(got_31, got_31, fsend.at[2]).wait()
    pb_wait(f_rs, 0, fsend)
    pb_wait(m_r, 1, fsend)
    pb_wait(f_all, 3, fsend)


def per_device(chol_vv, chol_ov, chol_oo, chol_vo, amplitudes):
    vv = chol_vv.reshape(QB * AB, NVIRT)
    ov = chol_ov.reshape(QB * JB, NVIRT)
    oo = chol_oo.reshape(QB * JB, NOCC)
    vo = chol_vo.transpose(0, 2, 1).reshape(QB * AB, NOCC)
    am = amplitudes.T
    dma = pltpu.SemaphoreType.DMA
    vv, ov, oo, vo, am = (pltpu.with_memory_space_constraint(x, pltpu.HBM) for x in (vv, ov, oo, vo, am))
    return pl.pallas_call(
        kernel,
        out_shape=(jax.ShapeDtypeStruct((QB, JB, NVIRT), BF), jax.ShapeDtypeStruct((JB, NVIRT), F32)),
        in_specs=[pl.BlockSpec(memory_space=pltpu.HBM)] * 5,
        out_specs=[pl.BlockSpec(memory_space=pltpu.VMEM)] * 2,
        scratch_shapes=[
            pltpu.VMEM((QB * AB, NVIRT), BF),
            pltpu.VMEM((QB * JB, NVIRT), BF),
            pltpu.VMEM((QB * JB, NOCC), BF),
            pltpu.VMEM((QB * AB, NOCC), BF),
            pltpu.VMEM((AB, NOCC), BF),
            pltpu.VMEM((AB // 8, 8, NOCC), BF),
            pltpu.VMEM((2, NPQ, AB // 8, 8, 128), BF),
            pltpu.VMEM((NVIRT, NOCC), BF),
            pltpu.VMEM((QB * JB, NOCC), BF),
            pltpu.VMEM((NPQ, 8, 1024), BF),
            pltpu.VMEM((2, NPQ, 8, 896), BF),
            pltpu.VMEM((NPQ, 8, 1024), BF),
            pltpu.VMEM((2, NPQ, 8, 896), BF),
            pltpu.VMEM((QB * 8, NOCC), F32),
            pltpu.VMEM((QB * 8, NVIRT), F32),
            pltpu.VMEM((1, 1, 128), F32),
            pltpu.VMEM((NPQ, 1, 128), F32),
            pltpu.VMEM((QB, 128), F32),
            pltpu.VMEM((QB, 8, 128), F32),
            pltpu.VMEM((NOCC, 128), F32),
            pltpu.VMEM((NPB, NPQ, 128), F32),
            pltpu.VMEM((NPB, NPQ, 128), F32),
            pltpu.VMEM((NPQ, 1, 128), F32),
            pltpu.VMEM((NPQ, 1, 128), F32),
            pltpu.VMEM((NPB, NPQ, 1, 128), F32),
            pltpu.VMEM((JB, NOCC), F32),
            pltpu.VMEM((NPB, JB, NOCC), F32),
            dma((5,)), dma, dma((NZ - 1,)), dma, dma((NY - 1,)), dma, dma((NY,)),
            dma((5,)), dma((5,)), dma, dma, dma((4,)), dma((4,)),
        ],
        compiler_params=pltpu.CompilerParams(
            collective_id=0, has_side_effects=True, vmem_limit_bytes=34 * 1024 * 1024),
    )(vv, ov, oo, vo, am)


def solution(mesh):
    in_specs = (
        P("pb", "pq", None),
        P("pb", "pq", None),
        P("pb", "pq", None),
        P("pb", None, "pq"),
        P(None, "pq"),
    )
    out_specs = (P("pb", "pq", None), P("pq", None))
    return jax.shard_map(
        per_device, mesh=mesh, in_specs=in_specs, out_specs=out_specs, check_vma=False
    )
```
